32 devices in a mesh: gz: 4 (over z), gy: 2 (over y), gx: 4 (over x, core).
Axes of the slice: x: 2, y: 2, z: 4, core: 2. Of those that a mesh axis runs over, the one named last changes fastest.
Arguments:
- velocity: float32 [3, 128, 32, 512], P(None, 'gx', 'gy', 'gz'), may hold values from -3.5 to 5.5
- pressure: float32 [128, 32, 512], P('gx', 'gy', 'gz'), may hold values from -6 to 6
- voidage: float32 [128, 32, 512], P('gx', 'gy', 'gz'), may hold values from 0.5 to 0.95
- particle_vel: float32 [3, 128, 32, 512], P(None, 'gx', 'gy', 'gz'), may hold values from -6 to 6
- forcing: float32 [1], replicated, may hold values from 0.5 to 2
- target_flux: float32 [1], replicated, may hold values from 0.5 to 1.5
Outputs:
- vel_new: float32 [3, 128, 32, 512], P(None, 'gx', 'gy', 'gz')
- source: float32 [128, 32, 512], P('gx', 'gy', 'gz')
- forcing_new: float32 [1], replicated
The draws below stay inside these ranges and needn't reach their ends.
All inputs are finite; a program needn't handle non-finite values.
Results may differ from the reference program's by a relative error of at most 0.000079.
Values sent between devices are 32-bit elements; how exact they have to be, the bound alone decides.
A program may use at most 64 MiB of HBM per device.

```python
import jax
import jax.numpy as jnp
from jax import lax

NX = 128
NY = 32
NZ = 512


def draw_velocity(key, part):
    jitter_field = jnp.clip(jax.random.normal(key, (3, NX, NY, NZ), jnp.float32), -3.5, 3.5)
    mean_lift = 2.0
    upward_mask = (jnp.arange(3) == 2).astype(jnp.float32).reshape(3, 1, 1, 1)
    return (jitter_field + mean_lift * upward_mask).astype(jnp.float32)


def levels(stream_key, shape, split, low, top_value):
    factor_of = 1.0
    for dim, shards_of in split:
        draws = jax.random.uniform(jax.random.fold_in(jax.random.fold_in(stream_key, 6), dim), (shards_of,), jnp.float32, low / len(split), top_value / len(split))
        factor_of = factor_of * jnp.repeat(jnp.exp(draws), shape[dim] // shards_of).reshape((-1,) + (1,) * (len(shape) - 1 - dim))
    return factor_of


def noise(key, extent, deviation, reach, split=(), kind=jnp.bfloat16):
    result = jax.random.normal(key, extent, jnp.float32) * deviation
    if len(split) > 0:
        result = levels(key, extent, split, -0.22, 0.18) * result
    return jnp.clip(result, min=-reach, max=reach).astype(kind)


def setup_inputs(seed: int = 0) -> dict:
    seeds = jax.random.split(jax.random.key(seed), 7)
    velocity = draw_velocity(jax.random.fold_in(seeds[6], 71), 0)
    pressure = noise(seeds[1], (NX, NY, NZ), 1.0, 6.0, ((0, 4), (1, 2), (2, 4)), jnp.float32)
    voidage = jnp.clip(0.5 + 0.45 * jax.random.uniform(seeds[2], (NX, NY, NZ), jnp.float32) ** levels(seeds[2], (NX, NY, NZ), ((0, 4), (1, 2), (2, 4)), -0.2, 0.2), 0.5, 0.95)
    particle_vel = noise(seeds[3], (3, NX, NY, NZ), 1.0, 6.0, ((1, 4), (2, 2), (3, 4)), jnp.float32)
    forcing = jnp.clip(jax.random.uniform(seeds[4], (1,), jnp.float32, 0.5, 2.0), 0.5, 2.0)
    target_flux = jnp.clip(jax.random.uniform(seeds[5], (1,), jnp.float32, 0.5, 1.5), 0.5, 1.5)
    return {"velocity": velocity, "pressure": pressure, "voidage": voidage, "particle_vel": particle_vel, "forcing": forcing, "target_flux": target_flux}


time_step = 0.2
viscosity = 0.1
drag_scale = 1.0

def shifted(field, axis_no, offset):
    slices = [slice(1, -1)] * 3
    length = field.shape[field.ndim - 3 + axis_no]
    slices[axis_no] = slice(1 + offset, length - 1 + offset)
    return field[tuple([slice(None)] * (field.ndim - 3) + slices)]

def upward():
    return (jnp.arange(3) == 2).astype(jnp.float32).reshape(3, 1, 1, 1)

def predict(vel_pad, pres_pad, voidage, particle_vel, forcing):
    centre = shifted(vel_pad, 0, 0)
    advection = jnp.zeros_like(centre)
    laplace = -6.0 * centre
    grads = []
    for axis_no in range(3):
        upper = shifted(vel_pad, axis_no, 1)
        lower = shifted(vel_pad, axis_no, -1)
        advection = advection + centre[axis_no] * (upper - lower) * 0.5
        laplace = laplace + upper + lower
        grads.append((shifted(pres_pad, axis_no, 1) - shifted(pres_pad, axis_no, -1)) * 0.5)
    forces = -advection + viscosity * laplace - jnp.stack(grads) + forcing * upward()
    slip_speed = jnp.sqrt(lax.optimization_barrier(jnp.sum((centre - particle_vel) ** 2, axis=0)))
    drag_rate = drag_scale * (1.0 - voidage) * voidage ** (-2.65) * (1.0 + slip_speed)
    return (centre + time_step * (forces + drag_rate * particle_vel)) / (1.0 + time_step * drag_rate)

def reference(velocity, pressure, voidage, particle_vel, forcing, target_flux):
    vel_pad = jnp.pad(velocity, ((0, 0), (1, 1), (1, 1), (0, 0)))
    vel_pad = jnp.pad(vel_pad, ((0, 0), (0, 0), (0, 0), (1, 1)), mode='wrap')
    pres_pad = jnp.pad(pressure, ((0, 0), (0, 0), (1, 1)), mode='wrap')
    pres_pad = jnp.pad(pres_pad, ((1, 1), (1, 1), (0, 0)), mode='edge')
    ustar = predict(vel_pad, pres_pad, voidage, particle_vel, forcing[0])
    flow_sum = jnp.sum(voidage * ustar[2])
    void_sum = jnp.sum(voidage)
    cells = voidage.size
    force_step = (target_flux[0] * cells - flow_sum) / (time_step * void_sum)
    vel_new = ustar + time_step * force_step * upward()
    flux = voidage * vel_new
    flux_pad = jnp.pad(flux, ((0, 0), (1, 1), (1, 1), (0, 0)))
    flux_pad = jnp.pad(flux_pad, ((0, 0), (0, 0), (0, 0), (1, 1)), mode='wrap')
    source = jnp.zeros_like(voidage)
    for axis_no in range(3):
        source = source + (shifted(flux_pad[axis_no], axis_no, 1) - shifted(flux_pad[axis_no], axis_no, -1)) * 0.5
    return (vel_new, source, forcing + force_step)
```

```python
import functools
import math

import jax
import jax.numpy as jnp
from jax import lax
from jax.experimental import pallas as pl
from jax.experimental.pallas import tpu as pltpu
from jax.sharding import PartitionSpec as P

time_step = 0.2
viscosity = 0.1
drag_scale = 1.0
MESH = pl.DeviceIdType.MESH
DIRECT_LIMIT = 0


def ring_index(axes):
    index = 0
    for axis in axes:
        index = index * lax.axis_size(axis) + lax.axis_index(axis)
    return index


def ring_device(axes, index):
    device = {}
    for axis in reversed(axes):
        size = lax.axis_size(axis)
        device[axis] = lax.rem(index, size)
        index = lax.div(index, size)
    return device


def kernel(
    sizes, phases,
    vel_hbm, pres_hbm, void_hbm, part_hbm, forcing, target,
    ustar, div, slope, step_out,
    blk, void, part, inv, flux, ypack, yhalo, zpack, zhalo,
    fypack, fyhalo, fxhalo, fzpack, fzhalo, slots,
    load_sem, send1, recv1, send2, recv2, sum_send, sum_recv,
):
    gx, gy, gz = sizes
    nx, ny, nz = div.shape
    x_at, y_at, z_at = (lax.axis_index(a) for a in ("gx", "gy", "gz"))
    not_low_x, not_high_x = x_at > 0, x_at < gx - 1
    not_low_y, not_high_y = y_at > 0, y_at < gy - 1
    z_up, z_down = lax.rem(z_at + 1, gz), lax.rem(z_at + gz - 1, gz)

    loads = [
        pltpu.make_async_copy(vel_hbm, blk.at[pl.ds(0, 3), pl.ds(1, nx)], load_sem.at[0]),
        pltpu.make_async_copy(pres_hbm, blk.at[3, pl.ds(1, nx)], load_sem.at[1]),
        pltpu.make_async_copy(void_hbm, void, load_sem.at[2]),
        pltpu.make_async_copy(part_hbm, part, load_sem.at[3]),
    ]
    for load in loads:
        load.start()

    barrier = pltpu.get_barrier_semaphore()
    peers = 0
    for axes in phases:
        count = math.prod(lax.axis_size(a) for a in axes)
        me = ring_index(axes)
        for k in range(1, count):
            pl.semaphore_signal(
                barrier, inc=1, device_id=ring_device(axes, lax.rem(me + k, count)),
                device_id_type=MESH,
            )
        peers += count - 1

    lane = lax.broadcasted_iota(jnp.int32, (ny, nz), 1)
    row = lax.broadcasted_iota(jnp.int32, (ny, nz), 0)

    def pack_z(fields, read, out):
        def body(x, carry):
            low, high = carry
            for f in range(fields):
                at = f * nx + x
                turned = pltpu.roll(read(f, x), at, 1)
                low = jnp.where(lane == at, turned, low)
                high = jnp.where(lane == lax.rem(at + nz - 1, nz), turned, high)
            return low, high

        zero = jnp.zeros((ny, nz), jnp.float32)
        low, high = lax.fori_loop(0, nx, body, (zero, zero), unroll=4)
        out[0] = low
        out[1] = high

    def copies(src_low, src_high, dst_low, dst_high, base, send, recv, axis, up, down):
        up_copy = pltpu.make_async_remote_copy(
            src_high, dst_low, send.at[base], recv.at[base],
            device_id={axis: up}, device_id_type=MESH)
        down_copy = pltpu.make_async_remote_copy(
            src_low, dst_high, send.at[base + 1], recv.at[base + 1],
            device_id={axis: down}, device_id_type=MESH)
        return up_copy, down_copy

    def start(pair, high, low):
        if high is None:
            pair[0].start()
            pair[1].start()
        else:
            pl.when(high)(pair[0].start)
            pl.when(low)(pair[1].start)

    def finish(pair, high, low):
        if high is None:
            pair[0].wait_recv()
            pair[1].wait_recv()
        else:
            pl.when(low)(pair[0].wait_recv)
            pl.when(high)(pair[1].wait_recv)

    def drain(pair, high, low):
        if high is None:
            pair[0].wait_send()
            pair[1].wait_send()
        else:
            pl.when(high)(pair[0].wait_send)
            pl.when(low)(pair[1].wait_send)

    up_x, down_x = jnp.minimum(x_at + 1, gx - 1), jnp.maximum(x_at - 1, 0)
    up_y, down_y = jnp.minimum(y_at + 1, gy - 1), jnp.maximum(y_at - 1, 0)

    loads[0].wait()
    loads[1].wait()
    for f in range(4):
        ypack[0, f] = blk[f, pl.ds(1, nx), 0, :]
        ypack[1, f] = blk[f, pl.ds(1, nx), ny - 1, :]
    pack_z(4, lambda f, x: blk[f, x + 1], zpack)
    pl.semaphore_wait(barrier, peers)

    y1 = copies(ypack.at[0], ypack.at[1], yhalo.at[0], yhalo.at[1], 0, send1, recv1, "gy", up_y, down_y)
    x1 = copies(blk.at[:, 1], blk.at[:, nx], blk.at[:, 0], blk.at[:, nx + 1], 2, send1, recv1, "gx", up_x, down_x)
    z1 = copies(zpack.at[0], zpack.at[1], zhalo.at[0], zhalo.at[1], 4, send1, recv1, "gz", z_up, z_down)
    start(z1, None, None)
    start(y1, not_high_y, not_low_y)
    start(x1, not_high_x, not_low_x)

    def wall_x(inside, halo_plane, edge_plane):
        @pl.when(jnp.logical_not(inside))
        def _():
            for f in range(3):
                blk[f, halo_plane] = jnp.zeros((ny, nz), jnp.float32)
            blk[3, halo_plane] = blk[3, edge_plane]

    wall_x(not_low_x, 0, 1)
    wall_x(not_high_x, nx + 1, nx)

    def wall_y(inside, side):
        @pl.when(jnp.logical_not(inside))
        def _():
            for f in range(3):
                yhalo[side, f] = jnp.zeros((nx, nz), jnp.float32)
            yhalo[side, 3] = ypack[side, 3]

    wall_y(not_low_y, 0)
    wall_y(not_high_y, 1)

    loads[2].wait()
    loads[3].wait()
    force = forcing[0]

    def plane(x):
        p = x + 1
        centre = [blk[f, p] for f in range(4)]
        v = void[x]
        q = [part[k, x] for k in range(3)]
        slip = jnp.sqrt(sum((centre[k] - q[k]) ** 2 for k in range(3)))
        drag = drag_scale * (1.0 - v) * jnp.exp(-2.65 * jnp.log(v)) * (1.0 + slip)
        inverse = 1.0 / (1.0 + time_step * drag)
        inv[x] = inverse

        def pair(f, axis_no):
            if axis_no == 0:
                return blk[f, p - 1], blk[f, p + 1]
            field = centre[f]
            if axis_no == 1:
                return (jnp.where(row == 0, 0.0, pltpu.roll(field, 1, 0)),
                        jnp.where(row == ny - 1, 0.0, pltpu.roll(field, ny - 1, 0)))
            return (jnp.where(lane == 0, 0.0, pltpu.roll(field, 1, 1)),
                    jnp.where(lane == nz - 1, 0.0, pltpu.roll(field, nz - 1, 1)))

        for k in range(3):
            advect = None
            total = None
            for axis_no in range(3):
                low, high = pair(k, axis_no)
                term = centre[axis_no] * (high - low)
                both = high + low
                advect = term if advect is None else advect + term
                total = both if total is None else total + both
            low, high = pair(3, k)
            forces = (viscosity * (total - 6.0 * centre[k])
                      - 0.5 * (advect + (high - low)))
            if k == 2:
                forces = forces + force
            ustar[k, x] = (centre[k] + time_step * (forces + drag * q[k])) * inverse

    def plane_body(i, carry):
        plane(1 + 2 * i)
        plane(2 + 2 * i)
        return carry

    lax.fori_loop(0, (nx - 2) // 2, plane_body, 0)

    finish(x1, not_high_x, not_low_x)
    plane(0)
    plane(nx - 1)

    finish(z1, None, None)
    finish(y1, not_high_y, not_low_y)

    first_row = row == 0
    last_row = row == ny - 1
    first_lane = lane == 0
    last_lane = lane == nz - 1
    row_sign = jnp.where(first_row, 1.0, jnp.where(last_row, -1.0, 0.0))
    lane_sign = jnp.where(first_lane, 1.0, jnp.where(last_lane, -1.0, 0.0))
    row_sign, lane_sign = (s * (0.5 * time_step) for s in (row_sign, lane_sign))
    row_visc, lane_visc = (jnp.abs(s) * (2.0 * viscosity) for s in (row_sign, lane_sign))

    def join_z(halo):
        low = pltpu.roll(halo[0], 1, 1)
        high = pltpu.roll(halo[1], nz - 1, 1)
        even = lax.rem(lane, 2) == 0
        return jnp.where(even, low, high), jnp.where(even, high, low)

    joined = join_z(zhalo)

    def unpack(which, at):
        return pltpu.roll(which, lax.rem(2 * nz - at, nz), 1)

    def correct(x, which, flow, void_total):
        inverse = inv[x]
        vy, vz = blk[1, x + 1], blk[2, x + 1]
        by_row = (row_visc + row_sign * vy) * inverse
        by_lane = (lane_visc + lane_sign * vz) * inverse

        def rows(f):
            return jnp.where(
                row < ny // 2,
                jnp.broadcast_to(yhalo[0, f, pl.ds(x, 1), :], (ny, nz)),
                jnp.broadcast_to(yhalo[1, f, pl.ds(x, 1), :], (ny, nz)))

        v = void[x]
        for k in range(3):
            value = ustar[k, x] + by_row * rows(k) + by_lane * unpack(which, k * nx + x)
            if k == 1:
                value = value + row_sign * inverse * rows(3)
            if k == 2:
                value = value + lane_sign * inverse * unpack(which, 3 * nx + x)
            ustar[k, x] = value
            moved = v * value
            flux[k, x] = moved
        return flow + moved, void_total + v

    def correct_body(i, carry):
        flow, void_total = carry
        flow, void_total = correct(2 * i, joined[0], flow, void_total)
        return correct(2 * i + 1, joined[1], flow, void_total)

    zero = jnp.zeros((ny, nz), jnp.float32)
    flow, void_total = lax.fori_loop(0, nx // 2, correct_body, (zero, zero))

    def fold(value):
        value = jnp.sum(value, axis=0, keepdims=True)
        return value + pltpu.roll(value, nz // 2, 1)

    line = lax.broadcasted_iota(jnp.int32, (1, nz), 1)
    partial = jnp.where(line < nz // 2, fold(flow), fold(void_total))

    def send_sum(which, value):
        axes = phases[which]
        count = math.prod(lax.axis_size(a) for a in axes)
        me = ring_index(axes)
        base = sum(math.prod(lax.axis_size(a) for a in phases[w]) for w in range(which))
        slots[base + me] = value
        out = []
        for k in range(1, count):
            out.append(pltpu.make_async_remote_copy(
                slots.at[base + me], slots.at[base + me],
                sum_send.at[base + k], sum_recv.at[base + me],
                device_id=ring_device(axes, lax.rem(me + k, count)), device_id_type=MESH))
            out[-1].start()
        return out

    def recv_sum(which):
        axes = phases[which]
        count = math.prod(lax.axis_size(a) for a in axes)
        me = ring_index(axes)
        base = sum(math.prod(lax.axis_size(a) for a in phases[w]) for w in range(which))
        for k in range(1, count):
            source = lax.rem(me + k, count)
            pltpu.make_async_remote_copy(
                slots.at[base + source], slots.at[base + source],
                sum_send.at[base + k], sum_recv.at[base + source],
                device_id=ring_device(axes, source), device_id_type=MESH).wait_recv()
        return jnp.sum(slots[pl.ds(base, count)], axis=0)

    sent = send_sum(0, partial)

    x2 = copies(flux.at[0, 0], flux.at[0, nx - 1], fxhalo.at[0], fxhalo.at[1], 0, send2, recv2, "gx", up_x, down_x)
    y2 = copies(fypack.at[0], fypack.at[1], fyhalo.at[0], fyhalo.at[1], 2, send2, recv2, "gy", up_y, down_y)
    z2 = copies(fzpack.at[0], fzpack.at[1], fzhalo.at[0], fzhalo.at[1], 4, send2, recv2, "gz", z_up, z_down)
    start(x2, not_high_x, not_low_x)
    fypack[0] = flux[1, :, 0, :]
    fypack[1] = flux[1, :, ny - 1, :]
    start(y2, not_high_y, not_low_y)
    pack_z(2, lambda f, x: flux[2, x] if f == 0 else void[x], fzpack)
    start(z2, None, None)

    for inside, side in ((not_low_x, 0), (not_high_x, 1)):
        @pl.when(jnp.logical_not(inside))
        def _():
            fxhalo[side] = jnp.zeros((ny, nz), jnp.float32)
    for inside, side in ((not_low_y, 0), (not_high_y, 1)):
        @pl.when(jnp.logical_not(inside))
        def _():
            fyhalo[side] = jnp.zeros((nx, nz), jnp.float32)

    phase = 0
    while phase < len(phases) - 1:
        total = recv_sum(phase)
        phase += 1
        sent += send_sum(phase, total)

    finish(x2, not_high_x, not_low_x)
    finish(y2, not_high_y, not_low_y)
    finish(z2, None, None)
    fz_joined = join_z(fzhalo)

    def source_plane(x, which, x_low, x_high):
        fy, fz, v = flux[1, x], flux[2, x], void[x]
        y_low = jnp.where(first_row, jnp.broadcast_to(fyhalo[0, pl.ds(x, 1), :], (ny, nz)), pltpu.roll(fy, 1, 0))
        y_high = jnp.where(last_row, jnp.broadcast_to(fyhalo[1, pl.ds(x, 1), :], (ny, nz)), pltpu.roll(fy, ny - 1, 0))
        z_halo, v_halo = unpack(which, x), unpack(which, nx + x)
        z_low = jnp.where(first_lane, z_halo, pltpu.roll(fz, 1, 1))
        z_high = jnp.where(last_lane, z_halo, pltpu.roll(fz, nz - 1, 1))
        v_low = jnp.where(first_lane, v_halo, pltpu.roll(v, 1, 1))
        v_high = jnp.where(last_lane, v_halo, pltpu.roll(v, nz - 1, 1))
        div[x] = 0.5 * ((x_high - x_low) + (y_high - y_low) + (z_high - z_low))
        slope[x] = (0.5 * time_step) * (v_high - v_low)

    source_plane(0, fz_joined[0], fxhalo[0], flux[0, 1])

    def source_body(i, carry):
        x = 2 * i + 1
        source_plane(x, fz_joined[1], flux[0, x - 1], flux[0, x + 1])
        source_plane(x + 1, fz_joined[0], flux[0, x], flux[0, x + 2])
        return carry

    lax.fori_loop(0, nx // 2 - 1, source_body, 0)
    source_plane(nx - 1, fz_joined[1], flux[0, nx - 2], fxhalo[1])

    total = recv_sum(phase)
    half = line < nz // 2
    flow_sum = jnp.sum(jnp.where(half, total, 0.0), axis=1, keepdims=True)
    void_sum = jnp.sum(jnp.where(half, 0.0, total), axis=1, keepdims=True)
    cells = float(nx * ny * nz * gx * gy * gz)
    step_out[...] = jnp.broadcast_to(
        (target[0] * cells - flow_sum) / (time_step * void_sum), (1, nz))

    for copy in sent:
        copy.wait_send()
    for pair, high, low in ((x1, not_high_x, not_low_x), (y1, not_high_y, not_low_y), (z1, None, None),
                            (x2, not_high_x, not_low_x), (y2, not_high_y, not_low_y), (z2, None, None)):
        drain(pair, high, low)


def local(velocity, pressure, voidage, particle_vel, forcing, target_flux):
    nx, ny, nz = voidage.shape
    sizes = tuple(lax.axis_size(a) for a in ("gx", "gy", "gz"))
    if math.prod(sizes) <= DIRECT_LIMIT:
        phases = (("gz", "gy", "gx"),)
    else:
        phases = (("gy", "gx"), ("gz",))
    slot_count = sum(math.prod(lax.axis_size(a) for a in axes) for axes in phases)
    f32 = jnp.float32
    vmem = pl.BlockSpec(memory_space=pltpu.VMEM)
    smem = pl.BlockSpec(memory_space=pltpu.SMEM)
    hbm = pl.BlockSpec(memory_space=pl.ANY)
    dma = pltpu.SemaphoreType.DMA
    ustar, div, slope, step = pl.pallas_call(
        functools.partial(kernel, sizes, phases),
        out_shape=(
            jax.ShapeDtypeStruct((3, nx, ny, nz), f32),
            jax.ShapeDtypeStruct((nx, ny, nz), f32),
            jax.ShapeDtypeStruct((nx, ny, nz), f32),
            jax.ShapeDtypeStruct((1, nz), f32),
        ),
        in_specs=[hbm, hbm, hbm, hbm, smem, smem],
        out_specs=(vmem, vmem, vmem, vmem),
        scratch_shapes=[
            pltpu.VMEM((4, nx + 2, ny, nz), f32),
            pltpu.VMEM((nx, ny, nz), f32),
            pltpu.VMEM((3, nx, ny, nz), f32),
            pltpu.VMEM((nx, ny, nz), f32),
            pltpu.VMEM((3, nx, ny, nz), f32),
            pltpu.VMEM((2, 4, nx, nz), f32),
            pltpu.VMEM((2, 4, nx, nz), f32),
            pltpu.VMEM((2, ny, nz), f32),
            pltpu.VMEM((2, ny, nz), f32),
            pltpu.VMEM((2, nx, nz), f32),
            pltpu.VMEM((2, nx, nz), f32),
            pltpu.VMEM((2, ny, nz), f32),
            pltpu.VMEM((2, ny, nz), f32),
            pltpu.VMEM((2, ny, nz), f32),
            pltpu.VMEM((slot_count, 1, nz), f32),
            dma((4,)), dma((6,)), dma((6,)), dma((6,)), dma((6,)),
            dma((slot_count,)), dma((slot_count,)),
        ],
        compiler_params=pltpu.CompilerParams(collective_id=0, has_side_effects=True),
    )(velocity, pressure, voidage, particle_vel, forcing, target_flux)
    force_step = step[0, :1]
    upward = (jnp.arange(3) == 2).astype(f32).reshape(3, 1, 1, 1)
    return (ustar + time_step * force_step[0] * upward, div + force_step[0] * slope, forcing + force_step)


def solution(mesh):
    return jax.shard_map(
        local,
        mesh=mesh,
        in_specs=(
            P(None, "gx", "gy", "gz"),
            P("gx", "gy", "gz"),
            P("gx", "gy", "gz"),
            P(None, "gx", "gy", "gz"),
            P(),
            P(),
        ),
        out_specs=(P(None, "gx", "gy", "gz"), P("gx", "gy", "gz"), P()),
        check_vma=False,
    )
```

```python
import functools
import math

import jax
import jax.numpy as jnp
from jax import lax
from jax.experimental import pallas as pl
from jax.experimental.pallas import tpu as pltpu
from jax.sharding import PartitionSpec as P

time_step = 0.2
viscosity = 0.1
drag_scale = 1.0
MESH = pl.DeviceIdType.MESH
DIRECT_LIMIT = 64


def ring_index(axes):
    index = 0
    for axis in axes:
        index = index * lax.axis_size(axis) + lax.axis_index(axis)
    return index


def ring_device(axes, index):
    device = {}
    for axis in reversed(axes):
        size = lax.axis_size(axis)
        device[axis] = lax.rem(index, size)
        index = lax.div(index, size)
    return device


def kernel(
    sizes, phases,
    vel_hbm, pres_hbm, void_hbm, part_hbm, forcing_hbm, target_hbm,
    ustar, div, step_out,
    forcing, target, slope,
    blk, void, part, inv, flux, ypack, yhalo, zpack, zhalo,
    fypack, fyhalo, fxhalo, fzpack, fzhalo, vzpack, vzhalo, slots,
    load_sem, send1, recv1, send2, recv2, sum_send, sum_recv,
):
    gx, gy, gz = sizes
    nx, ny, nz = div.shape
    x_at, y_at, z_at = (lax.axis_index(a) for a in ("gx", "gy", "gz"))
    not_low_x, not_high_x = x_at > 0, x_at < gx - 1
    not_low_y, not_high_y = y_at > 0, y_at < gy - 1
    z_up, z_down = lax.rem(z_at + 1, gz), lax.rem(z_at + gz - 1, gz)

    loads = [
        pltpu.make_async_copy(vel_hbm, blk.at[pl.ds(0, 3), pl.ds(1, nx)], load_sem.at[0]),
        pltpu.make_async_copy(pres_hbm, blk.at[3, pl.ds(1, nx)], load_sem.at[1]),
        pltpu.make_async_copy(void_hbm, void, load_sem.at[2]),
        pltpu.make_async_copy(part_hbm, part, load_sem.at[3]),
        pltpu.make_async_copy(forcing_hbm, forcing, load_sem.at[4]),
        pltpu.make_async_copy(target_hbm, target, load_sem.at[5]),
    ]
    for load in loads:
        load.start()

    barrier = pltpu.get_barrier_semaphore()
    peers = 0
    for axes in phases:
        count = math.prod(lax.axis_size(a) for a in axes)
        me = ring_index(axes)
        for k in range(1, count):
            pl.semaphore_signal(
                barrier, inc=1, device_id=ring_device(axes, lax.rem(me + k, count)),
                device_id_type=MESH,
            )
        peers += count - 1

    lane = lax.broadcasted_iota(jnp.int32, (ny, nz), 1)
    row = lax.broadcasted_iota(jnp.int32, (ny, nz), 0)

    def pack_z(fields, read, out):
        def body(x, carry):
            low, high = carry
            for f in range(fields):
                at = f * nx + x
                turned = pltpu.roll(read(f, x), at, 1)
                low = jnp.where(lane == at, turned, low)
                high = jnp.where(lane == lax.rem(at + nz - 1, nz), turned, high)
            return low, high

        zero = jnp.zeros((ny, nz), jnp.float32)
        low, high = lax.fori_loop(0, nx, body, (zero, zero), unroll=4)
        out[0] = low
        out[1] = high

    def copies(src_low, src_high, dst_low, dst_high, base, send, recv, axis, up, down):
        up_copy = pltpu.make_async_remote_copy(
            src_high, dst_low, send.at[base], recv.at[base],
            device_id={axis: up}, device_id_type=MESH)
        down_copy = pltpu.make_async_remote_copy(
            src_low, dst_high, send.at[base + 1], recv.at[base + 1],
            device_id={axis: down}, device_id_type=MESH)
        return up_copy, down_copy

    def start(pair, high, low):
        if high is None:
            pair[0].start()
            pair[1].start()
        else:
            pl.when(high)(pair[0].start)
            pl.when(low)(pair[1].start)

    def finish(pair, high, low):
        if high is None:
            pair[0].wait_recv()
            pair[1].wait_recv()
        else:
            pl.when(low)(pair[0].wait_recv)
            pl.when(high)(pair[1].wait_recv)

    def drain(pair, high, low):
        if high is None:
            pair[0].wait_send()
            pair[1].wait_send()
        else:
            pl.when(high)(pair[0].wait_send)
            pl.when(low)(pair[1].wait_send)

    up_x, down_x = jnp.minimum(x_at + 1, gx - 1), jnp.maximum(x_at - 1, 0)
    up_y, down_y = jnp.minimum(y_at + 1, gy - 1), jnp.maximum(y_at - 1, 0)

    loads[0].wait()
    loads[1].wait()
    for f in range(4):
        ypack[0, f] = blk[f, pl.ds(1, nx), 0, :]
        ypack[1, f] = blk[f, pl.ds(1, nx), ny - 1, :]
    pack_z(4, lambda f, x: blk[f, x + 1], zpack)
    pl.semaphore_wait(barrier, peers)

    y1 = copies(ypack.at[0], ypack.at[1], yhalo.at[0], yhalo.at[1], 0, send1, recv1, "gy", up_y, down_y)
    x1 = copies(blk.at[:, 1], blk.at[:, nx], blk.at[:, 0], blk.at[:, nx + 1], 2, send1, recv1, "gx", up_x, down_x)
    z1 = copies(zpack.at[0], zpack.at[1], zhalo.at[0], zhalo.at[1], 4, send1, recv1, "gz", z_up, z_down)
    start(z1, None, None)
    start(y1, not_high_y, not_low_y)
    start(x1, not_high_x, not_low_x)

    def wall_x(inside, halo_plane, edge_plane):
        @pl.when(jnp.logical_not(inside))
        def _():
            for f in range(3):
                blk[f, halo_plane] = jnp.zeros((ny, nz), jnp.float32)
            blk[3, halo_plane] = blk[3, edge_plane]

    wall_x(not_low_x, 0, 1)
    wall_x(not_high_x, nx + 1, nx)

    def wall_y(inside, side):
        @pl.when(jnp.logical_not(inside))
        def _():
            for f in range(3):
                yhalo[side, f] = jnp.zeros((nx, nz), jnp.float32)
            yhalo[side, 3] = ypack[side, 3]

    wall_y(not_low_y, 0)
    wall_y(not_high_y, 1)

    loads[2].wait()
    loads[3].wait()
    loads[4].wait()
    loads[5].wait()
    force = forcing[0]

    def plane(x):
        p = x + 1
        centre = [blk[f, p] for f in range(4)]
        v = void[x]
        q = [part[k, x] for k in range(3)]
        slip = jnp.sqrt(sum((centre[k] - q[k]) ** 2 for k in range(3)))
        drag = drag_scale * (1.0 - v) * jnp.exp(-2.65 * jnp.log(v)) * (1.0 + slip)
        inverse = 1.0 / (1.0 + time_step * drag)
        inv[x] = inverse

        def pair(f, axis_no):
            if axis_no == 0:
                return blk[f, p - 1], blk[f, p + 1]
            field = centre[f]
            if axis_no == 1:
                return (jnp.where(row == 0, 0.0, pltpu.roll(field, 1, 0)),
                        jnp.where(row == ny - 1, 0.0, pltpu.roll(field, ny - 1, 0)))
            return (jnp.where(lane == 0, 0.0, pltpu.roll(field, 1, 1)),
                    jnp.where(lane == nz - 1, 0.0, pltpu.roll(field, nz - 1, 1)))

        for k in range(3):
            advect = None
            total = None
            for axis_no in range(3):
                low, high = pair(k, axis_no)
                term = centre[axis_no] * (high - low)
                both = high + low
                advect = term if advect is None else advect + term
                total = both if total is None else total + both
            low, high = pair(3, k)
            forces = (viscosity * (total - 6.0 * centre[k])
                      - 0.5 * (advect + (high - low)))
            if k == 2:
                forces = forces + force
            ustar[k, x] = (centre[k] + time_step * (forces + drag * q[k])) * inverse

    def plane_body(i, carry):
        plane(1 + 2 * i)
        plane(2 + 2 * i)
        return carry

    lax.fori_loop(0, (nx - 2) // 2, plane_body, 0)

    pack_z(1, lambda f, x: void[x], vzpack)
    zv = copies(vzpack.at[0], vzpack.at[1], vzhalo.at[0], vzhalo.at[1], 6, send1, recv1, "gz", z_up, z_down)
    start(zv, None, None)

    finish(x1, not_high_x, not_low_x)
    plane(0)
    plane(nx - 1)

    finish(z1, None, None)
    finish(y1, not_high_y, not_low_y)

    first_row = row == 0
    last_row = row == ny - 1
    first_lane = lane == 0
    last_lane = lane == nz - 1
    row_sign = jnp.where(first_row, 1.0, jnp.where(last_row, -1.0, 0.0))
    lane_sign = jnp.where(first_lane, 1.0, jnp.where(last_lane, -1.0, 0.0))
    row_sign, lane_sign = (s * (0.5 * time_step) for s in (row_sign, lane_sign))
    row_visc, lane_visc = (jnp.abs(s) * (2.0 * viscosity) for s in (row_sign, lane_sign))

    def join_z(halo):
        low = pltpu.roll(halo[0], 1, 1)
        high = pltpu.roll(halo[1], nz - 1, 1)
        even = lax.rem(lane, 2) == 0
        return jnp.where(even, low, high), jnp.where(even, high, low)

    joined = join_z(zhalo)

    def unpack(which, at):
        return pltpu.roll(which, lax.rem(2 * nz - at, nz), 1)

    def rows(f, x):
        return jnp.where(
            row < ny // 2,
            jnp.broadcast_to(yhalo[0, f, pl.ds(x, 1), :], (ny, nz)),
            jnp.broadcast_to(yhalo[1, f, pl.ds(x, 1), :], (ny, nz)))

    def correct(x, which, fields):
        by_row = row_visc + row_sign * blk[1, x + 1]
        by_lane = lane_visc + lane_sign * blk[2, x + 1]
        inverse, v = inv[x], void[x]
        for k in fields:
            value = by_row * rows(k, x) + by_lane * unpack(which, k * nx + x)
            if k == 1:
                value = value + row_sign * rows(3, x)
            if k == 2:
                value = value + lane_sign * unpack(which, 3 * nx + x)
            value = ustar[k, x] + value * inverse
            ustar[k, x] = value
            moved = v * value
            flux[k, x] = moved
        return moved, v

    def flow_body(i, carry):
        flow, void_total = carry
        for x, which in ((2 * i, joined[0]), (2 * i + 1, joined[1])):
            moved, v = correct(x, which, (2,))
            flow, void_total = flow + moved, void_total + v
        return flow, void_total

    def across_body(i, carry):
        correct(2 * i, joined[0], (0, 1))
        correct(2 * i + 1, joined[1], (0, 1))
        return carry

    zero = jnp.zeros((ny, nz), jnp.float32)
    flow, void_total = lax.fori_loop(0, nx // 2, flow_body, (zero, zero))

    def fold(value):
        value = jnp.sum(value, axis=0, keepdims=True)
        return value + pltpu.roll(value, nz // 2, 1)

    line = lax.broadcasted_iota(jnp.int32, (1, nz), 1)
    partial = jnp.where(line < nz // 2, fold(flow), fold(void_total))

    def send_sum(which, value):
        axes = phases[which]
        count = math.prod(lax.axis_size(a) for a in axes)
        me = ring_index(axes)
        base = sum(math.prod(lax.axis_size(a) for a in phases[w]) for w in range(which))
        slots[base + me] = value
        out = []
        for k in range(1, count):
            out.append(pltpu.make_async_remote_copy(
                slots.at[base + me], slots.at[base + me],
                sum_send.at[base + k], sum_recv.at[base + me],
                device_id=ring_device(axes, lax.rem(me + k, count)), device_id_type=MESH))
            out[-1].start()
        return out

    def recv_sum(which):
        axes = phases[which]
        count = math.prod(lax.axis_size(a) for a in axes)
        me = ring_index(axes)
        base = sum(math.prod(lax.axis_size(a) for a in phases[w]) for w in range(which))
        for k in range(1, count):
            source = lax.rem(me + k, count)
            pltpu.make_async_remote_copy(
                slots.at[base + source], slots.at[base + source],
                sum_send.at[base + k], sum_recv.at[base + source],
                device_id=ring_device(axes, source), device_id_type=MESH).wait_recv()
        return jnp.sum(slots[pl.ds(base, count)], axis=0)

    sent = send_sum(0, partial)

    x2 = copies(flux.at[0, 0], flux.at[0, nx - 1], fxhalo.at[0], fxhalo.at[1], 0, send2, recv2, "gx", up_x, down_x)
    y2 = copies(fypack.at[0], fypack.at[1], fyhalo.at[0], fyhalo.at[1], 2, send2, recv2, "gy", up_y, down_y)
    z2 = copies(fzpack.at[0], fzpack.at[1], fzhalo.at[0], fzhalo.at[1], 4, send2, recv2, "gz", z_up, z_down)
    pack_z(1, lambda f, x: flux[2, x], fzpack)
    start(z2, None, None)
    lax.fori_loop(0, nx // 2, across_body, 0)
    start(x2, not_high_x, not_low_x)
    fypack[0] = flux[1, :, 0, :]
    fypack[1] = flux[1, :, ny - 1, :]
    start(y2, not_high_y, not_low_y)

    for inside, side in ((not_low_x, 0), (not_high_x, 1)):
        @pl.when(jnp.logical_not(inside))
        def _():
            fxhalo[side] = jnp.zeros((ny, nz), jnp.float32)
    for inside, side in ((not_low_y, 0), (not_high_y, 1)):
        @pl.when(jnp.logical_not(inside))
        def _():
            fyhalo[side] = jnp.zeros((nx, nz), jnp.float32)

    phase = 0
    while phase < len(phases) - 1:
        total = recv_sum(phase)
        phase += 1
        sent += send_sum(phase, total)

    finish(x2, not_high_x, not_low_x)
    finish(y2, not_high_y, not_low_y)
    finish(z2, None, None)
    finish(zv, None, None)
    fz_joined = join_z(fzhalo)
    vz_joined = join_z(vzhalo)

    def source_plane(x, odd, x_low, x_high):
        fy, fz, v = flux[1, x], flux[2, x], void[x]
        y_low = jnp.where(first_row, jnp.broadcast_to(fyhalo[0, pl.ds(x, 1), :], (ny, nz)), pltpu.roll(fy, 1, 0))
        y_high = jnp.where(last_row, jnp.broadcast_to(fyhalo[1, pl.ds(x, 1), :], (ny, nz)), pltpu.roll(fy, ny - 1, 0))
        z_halo, v_halo = unpack(fz_joined[odd], x), unpack(vz_joined[odd], x)
        z_low = jnp.where(first_lane, z_halo, pltpu.roll(fz, 1, 1))
        z_high = jnp.where(last_lane, z_halo, pltpu.roll(fz, nz - 1, 1))
        v_low = jnp.where(first_lane, v_halo, pltpu.roll(v, 1, 1))
        v_high = jnp.where(last_lane, v_halo, pltpu.roll(v, nz - 1, 1))
        div[x] = 0.5 * ((x_high - x_low) + (y_high - y_low) + (z_high - z_low))
        slope[x] = (0.5 * time_step) * (v_high - v_low)

    source_plane(0, 0, fxhalo[0], flux[0, 1])

    def source_body(i, carry):
        x = 2 * i + 1
        source_plane(x, 1, flux[0, x - 1], flux[0, x + 1])
        source_plane(x + 1, 0, flux[0, x], flux[0, x + 2])
        return carry

    lax.fori_loop(0, nx // 2 - 1, source_body, 0)
    source_plane(nx - 1, 1, flux[0, nx - 2], fxhalo[1])

    total = recv_sum(phase)
    half = line < nz // 2
    flow_sum = jnp.sum(jnp.where(half, total, 0.0), axis=1, keepdims=True)
    void_sum = jnp.sum(jnp.where(half, 0.0, total), axis=1, keepdims=True)
    cells = float(nx * ny * nz * gx * gy * gz)
    step = (target[0] * cells - flow_sum) / (time_step * void_sum)
    step_out[...] = jnp.broadcast_to(step, (1, nz)) + forcing[0]
    step = jnp.broadcast_to(step, (ny, nz))

    def final_body(x, carry):
        ustar[2, x] = ustar[2, x] + time_step * step
        div[x] = div[x] + step * slope[x]
        return carry

    lax.fori_loop(0, nx, final_body, 0, unroll=4)

    for copy in sent:
        copy.wait_send()
    for pair, high, low in ((x1, not_high_x, not_low_x), (y1, not_high_y, not_low_y), (z1, None, None), (zv, None, None),
                            (x2, not_high_x, not_low_x), (y2, not_high_y, not_low_y), (z2, None, None)):
        drain(pair, high, low)


def local(velocity, pressure, voidage, particle_vel, forcing, target_flux):
    nx, ny, nz = voidage.shape
    sizes = tuple(lax.axis_size(a) for a in ("gx", "gy", "gz"))
    if math.prod(sizes) <= DIRECT_LIMIT:
        phases = (("gz", "gy", "gx"),)
    else:
        phases = (("gy", "gx"), ("gz",))
    slot_count = sum(math.prod(lax.axis_size(a) for a in axes) for axes in phases)
    f32 = jnp.float32
    vmem = pl.BlockSpec(memory_space=pltpu.VMEM)
    hbm = pl.BlockSpec(memory_space=pltpu.HBM)
    dma = pltpu.SemaphoreType.DMA
    vel_new, source, forcing_new = pl.pallas_call(
        functools.partial(kernel, sizes, phases),
        out_shape=(
            pltpu.VMEM((3, nx, ny, nz), f32),
            pltpu.VMEM((nx, ny, nz), f32),
            pltpu.VMEM((1, nz), f32),
        ),
        in_specs=[hbm] * 6,
        out_specs=(vmem,) * 3,
        scratch_shapes=[
            pltpu.SMEM((1,), f32),
            pltpu.SMEM((1,), f32),
            pltpu.VMEM((nx, ny, nz), f32),
            pltpu.VMEM((4, nx + 2, ny, nz), f32),
            pltpu.VMEM((nx, ny, nz), f32),
            pltpu.VMEM((3, nx, ny, nz), f32),
            pltpu.VMEM((nx, ny, nz), f32),
            pltpu.VMEM((3, nx, ny, nz), f32),
            pltpu.VMEM((2, 4, nx, nz), f32),
            pltpu.VMEM((2, 4, nx, nz), f32),
            pltpu.VMEM((2, ny, nz), f32),
            pltpu.VMEM((2, ny, nz), f32),
            pltpu.VMEM((2, nx, nz), f32),
            pltpu.VMEM((2, nx, nz), f32),
            pltpu.VMEM((2, ny, nz), f32),
            pltpu.VMEM((2, ny, nz), f32),
            pltpu.VMEM((2, ny, nz), f32),
            pltpu.VMEM((2, ny, nz), f32),
            pltpu.VMEM((2, ny, nz), f32),
            pltpu.VMEM((slot_count, 1, nz), f32),
            dma((6,)), dma((8,)), dma((8,)), dma((6,)), dma((6,)),
            dma((slot_count,)), dma((slot_count,)),
        ],
        compiler_params=pltpu.CompilerParams(collective_id=0, has_side_effects=True),
    )(velocity, pressure, voidage, particle_vel, forcing, target_flux)
    return vel_new, source, forcing_new[0, :1]


def solution(mesh):
    return jax.shard_map(
        local,
        mesh=mesh,
        in_specs=(
            P(None, "gx", "gy", "gz"),
            P("gx", "gy", "gz"),
            P("gx", "gy", "gz"),
            P(None, "gx", "gy", "gz"),
            P(),
            P(),
        ),
        out_specs=(P(None, "gx", "gy", "gz"), P("gx", "gy", "gz"), P()),
        check_vma=False,
    )
```

```python
import functools
import math

import jax
import jax.numpy as jnp
from jax import lax
from jax.experimental import pallas as pl
from jax.experimental.pallas import tpu as pltpu
from jax.sharding import PartitionSpec as P

time_step = 0.2
viscosity = 0.1
drag_scale = 1.0
MESH = pl.DeviceIdType.MESH
DIRECT_LIMIT = 64


def ring_index(axes):
    index = 0
    for axis in axes:
        index = index * lax.axis_size(axis) + lax.axis_index(axis)
    return index


def ring_device(axes, index):
    device = {}
    for axis in reversed(axes):
        size = lax.axis_size(axis)
        device[axis] = lax.rem(index, size)
        index = lax.div(index, size)
    return device


def kernel(
    sizes, greet, phases,
    vel_hbm, pres_hbm, void_hbm, part_hbm, forcing_hbm, target_hbm,
    ustar, div, step_out,
    forcing, target, slope,
    blk, void, part, inv, flux, ypack, yhalo, zpack, zhalo,
    fypack, fyhalo, fxhalo, fzpack, fzhalo, vzpack, vzhalo, slots,
    load_sem, send1, recv1, send2, recv2, sum_send, sum_recv, entered,
):
    gx, gy, gz = sizes
    nx, ny, nz = div.shape
    x_at, y_at, z_at = (lax.axis_index(a) for a in ("gx", "gy", "gz"))
    not_low_x, not_high_x = x_at > 0, x_at < gx - 1
    not_low_y, not_high_y = y_at > 0, y_at < gy - 1
    z_up, z_down = lax.rem(z_at + 1, gz), lax.rem(z_at + gz - 1, gz)

    loads = [
        pltpu.make_async_copy(vel_hbm, blk.at[pl.ds(0, 3), pl.ds(1, nx)], load_sem.at[0]),
        pltpu.make_async_copy(pres_hbm, blk.at[3, pl.ds(1, nx)], load_sem.at[1]),
        pltpu.make_async_copy(void_hbm, void, load_sem.at[2]),
        pltpu.make_async_copy(part_hbm, part, load_sem.at[3]),
        pltpu.make_async_copy(forcing_hbm, forcing, load_sem.at[4]),
        pltpu.make_async_copy(target_hbm, target, load_sem.at[5]),
    ]
    for load in loads:
        load.start()

    barrier = pltpu.get_barrier_semaphore()
    peers = 0
    for axes in greet:
        count = math.prod(lax.axis_size(a) for a in axes)
        me = ring_index(axes)
        for k in range(1, count):
            pl.semaphore_signal(
                barrier, inc=1, device_id=ring_device(axes, lax.rem(me + k, count)),
                device_id_type=MESH,
            )
        peers += count - 1

    lane = lax.broadcasted_iota(jnp.int32, (ny, nz), 1)
    row = lax.broadcasted_iota(jnp.int32, (ny, nz), 0)

    def pack_z(fields, read, out):
        def body(x, carry):
            low, high = carry
            for f in range(fields):
                at = f * nx + x
                turned = pltpu.roll(read(f, x), at, 1)
                low = jnp.where(lane == at, turned, low)
                high = jnp.where(lane == lax.rem(at + nz - 1, nz), turned, high)
            return low, high

        zero = jnp.zeros((ny, nz), jnp.float32)
        low, high = lax.fori_loop(0, nx, body, (zero, zero), unroll=4)
        out[0] = low
        out[1] = high

    def copies(src_low, src_high, dst_low, dst_high, base, send, recv, axis, up, down):
        up_copy = pltpu.make_async_remote_copy(
            src_high, dst_low, send.at[base], recv.at[base],
            device_id={axis: up}, device_id_type=MESH)
        down_copy = pltpu.make_async_remote_copy(
            src_low, dst_high, send.at[base + 1], recv.at[base + 1],
            device_id={axis: down}, device_id_type=MESH)
        return up_copy, down_copy

    def start(pair, high, low):
        if high is None:
            pair[0].start()
            pair[1].start()
        else:
            pl.when(high)(pair[0].start)
            pl.when(low)(pair[1].start)

    def finish(pair, high, low):
        if high is None:
            pair[0].wait_recv()
            pair[1].wait_recv()
        else:
            pl.when(low)(pair[0].wait_recv)
            pl.when(high)(pair[1].wait_recv)

    def drain(pair, high, low):
        if high is None:
            pair[0].wait_send()
            pair[1].wait_send()
        else:
            pl.when(high)(pair[0].wait_send)
            pl.when(low)(pair[1].wait_send)

    up_x, down_x = jnp.minimum(x_at + 1, gx - 1), jnp.maximum(x_at - 1, 0)
    up_y, down_y = jnp.minimum(y_at + 1, gy - 1), jnp.maximum(y_at - 1, 0)

    loads[0].wait()
    loads[1].wait()
    for f in range(4):
        ypack[0, f] = blk[f, pl.ds(1, nx), 0, :]
        ypack[1, f] = blk[f, pl.ds(1, nx), ny - 1, :]
    pack_z(4, lambda f, x: blk[f, x + 1], zpack)
    loads[2].wait()
    loads[3].wait()
    loads[4].wait()
    loads[5].wait()
    force = forcing[0]

    def plane(x):
        p = x + 1
        centre = [blk[f, p] for f in range(4)]
        v = void[x]
        q = [part[k, x] for k in range(3)]
        slip = jnp.sqrt(sum((centre[k] - q[k]) ** 2 for k in range(3)))
        drag = drag_scale * (1.0 - v) * jnp.exp(-2.65 * jnp.log(v)) * (1.0 + slip)
        inverse = 1.0 / (1.0 + time_step * drag)
        inv[x] = inverse

        def pair(f, axis_no):
            if axis_no == 0:
                return blk[f, p - 1], blk[f, p + 1]
            field = centre[f]
            if axis_no == 1:
                return (jnp.where(row == 0, 0.0, pltpu.roll(field, 1, 0)),
                        jnp.where(row == ny - 1, 0.0, pltpu.roll(field, ny - 1, 0)))
            return (jnp.where(lane == 0, 0.0, pltpu.roll(field, 1, 1)),
                    jnp.where(lane == nz - 1, 0.0, pltpu.roll(field, nz - 1, 1)))

        for k in range(3):
            advect = None
            total = None
            for axis_no in range(3):
                low, high = pair(k, axis_no)
                term = centre[axis_no] * (high - low)
                both = high + low
                advect = term if advect is None else advect + term
                total = both if total is None else total + both
            low, high = pair(3, k)
            forces = (viscosity * (total - 6.0 * centre[k])
                      - 0.5 * (advect + (high - low)))
            if k == 2:
                forces = forces + force
            ustar[k, x] = (centre[k] + time_step * (forces + drag * q[k])) * inverse

    def plane_body(i, carry):
        plane(1 + 2 * i)
        plane(2 + 2 * i)
        return carry

    pack_z(1, lambda f, x: void[x], vzpack)
    early = (nx - 2) // 4
    lax.fori_loop(0, early, plane_body, 0)
    pl.semaphore_wait(barrier, peers)

    y1 = copies(ypack.at[0], ypack.at[1], yhalo.at[0], yhalo.at[1], 0, send1, recv1, "gy", up_y, down_y)
    x1 = copies(blk.at[:, 1], blk.at[:, nx], blk.at[:, 0], blk.at[:, nx + 1], 2, send1, recv1, "gx", up_x, down_x)
    z1 = copies(zpack.at[0], zpack.at[1], zhalo.at[0], zhalo.at[1], 4, send1, recv1, "gz", z_up, z_down)
    start(z1, None, None)
    start(y1, not_high_y, not_low_y)
    start(x1, not_high_x, not_low_x)
    zv = copies(vzpack.at[0], vzpack.at[1], vzhalo.at[0], vzhalo.at[1], 6, send1, recv1, "gz", z_up, z_down)
    start(zv, None, None)

    spread = len(phases) < len(greet)
    if spread:
        for k in range(1, gz):
            pl.semaphore_signal(
                entered, inc=1, device_id={"gz": lax.rem(z_at + k, gz)}, device_id_type=MESH)

    def wall_x(inside, halo_plane, edge_plane):
        @pl.when(jnp.logical_not(inside))
        def _():
            for f in range(3):
                blk[f, halo_plane] = jnp.zeros((ny, nz), jnp.float32)
            blk[3, halo_plane] = blk[3, edge_plane]

    wall_x(not_low_x, 0, 1)
    wall_x(not_high_x, nx + 1, nx)

    def wall_y(inside, side):
        @pl.when(jnp.logical_not(inside))
        def _():
            for f in range(3):
                yhalo[side, f] = jnp.zeros((nx, nz), jnp.float32)
            yhalo[side, 3] = ypack[side, 3]

    wall_y(not_low_y, 0)
    wall_y(not_high_y, 1)

    lax.fori_loop(early, (nx - 2) // 2, plane_body, 0)


    finish(x1, not_high_x, not_low_x)
    plane(0)
    plane(nx - 1)

    finish(z1, None, None)
    finish(y1, not_high_y, not_low_y)

    first_row = row == 0
    last_row = row == ny - 1
    first_lane = lane == 0
    last_lane = lane == nz - 1
    row_sign = jnp.where(first_row, 1.0, jnp.where(last_row, -1.0, 0.0))
    lane_sign = jnp.where(first_lane, 1.0, jnp.where(last_lane, -1.0, 0.0))
    row_sign, lane_sign = (s * (0.5 * time_step) for s in (row_sign, lane_sign))
    row_visc, lane_visc = (jnp.abs(s) * (2.0 * viscosity) for s in (row_sign, lane_sign))

    def join_z(halo):
        low = pltpu.roll(halo[0], 1, 1)
        high = pltpu.roll(halo[1], nz - 1, 1)
        even = lax.rem(lane, 2) == 0
        return jnp.where(even, low, high), jnp.where(even, high, low)

    joined = join_z(zhalo)

    def unpack(which, at):
        return pltpu.roll(which, lax.rem(2 * nz - at, nz), 1)

    def rows(f, x):
        return jnp.where(
            row < ny // 2,
            jnp.broadcast_to(yhalo[0, f, pl.ds(x, 1), :], (ny, nz)),
            jnp.broadcast_to(yhalo[1, f, pl.ds(x, 1), :], (ny, nz)))

    def correct(x, which, fields):
        by_row = row_visc + row_sign * blk[1, x + 1]
        by_lane = lane_visc + lane_sign * blk[2, x + 1]
        inverse, v = inv[x], void[x]
        for k in fields:
            value = by_row * rows(k, x) + by_lane * unpack(which, k * nx + x)
            if k == 1:
                value = value + row_sign * rows(3, x)
            if k == 2:
                value = value + lane_sign * unpack(which, 3 * nx + x)
            value = ustar[k, x] + value * inverse
            ustar[k, x] = value
            moved = v * value
            flux[k, x] = moved
        return moved, v

    def flow_body(i, carry):
        flow, void_total = carry
        for x, which in ((2 * i, joined[0]), (2 * i + 1, joined[1])):
            moved, v = correct(x, which, (2,))
            flow, void_total = flow + moved, void_total + v
        return flow, void_total

    def across_body(i, carry):
        correct(2 * i, joined[0], (0, 1))
        correct(2 * i + 1, joined[1], (0, 1))
        return carry

    zero = jnp.zeros((ny, nz), jnp.float32)
    flow, void_total = lax.fori_loop(0, nx // 2, flow_body, (zero, zero))

    def fold(value):
        value = jnp.sum(value, axis=0, keepdims=True)
        return value + pltpu.roll(value, nz // 2, 1)

    line = lax.broadcasted_iota(jnp.int32, (1, nz), 1)
    partial = jnp.where(line < nz // 2, fold(flow), fold(void_total))

    if spread:
        pl.semaphore_wait(entered, gz - 1)

    def send_sum(which, value):
        axes = phases[which]
        count = math.prod(lax.axis_size(a) for a in axes)
        me = ring_index(axes)
        base = sum(math.prod(lax.axis_size(a) for a in phases[w]) for w in range(which))
        slots[base + me] = value
        out = []
        for k in range(1, count):
            out.append(pltpu.make_async_remote_copy(
                slots.at[base + me], slots.at[base + me],
                sum_send.at[base + k], sum_recv.at[base + me],
                device_id=ring_device(axes, lax.rem(me + k, count)), device_id_type=MESH))
            out[-1].start()
        return out

    def recv_sum(which):
        axes = phases[which]
        count = math.prod(lax.axis_size(a) for a in axes)
        me = ring_index(axes)
        base = sum(math.prod(lax.axis_size(a) for a in phases[w]) for w in range(which))
        for k in range(1, count):
            source = lax.rem(me + k, count)
            pltpu.make_async_remote_copy(
                slots.at[base + source], slots.at[base + source],
                sum_send.at[base + k], sum_recv.at[base + source],
                device_id=ring_device(axes, source), device_id_type=MESH).wait_recv()
        return jnp.sum(slots[pl.ds(base, count)], axis=0)

    sent = send_sum(0, partial)

    x2 = copies(flux.at[0, 0], flux.at[0, nx - 1], fxhalo.at[0], fxhalo.at[1], 0, send2, recv2, "gx", up_x, down_x)
    y2 = copies(fypack.at[0], fypack.at[1], fyhalo.at[0], fyhalo.at[1], 2, send2, recv2, "gy", up_y, down_y)
    z2 = copies(fzpack.at[0], fzpack.at[1], fzhalo.at[0], fzhalo.at[1], 4, send2, recv2, "gz", z_up, z_down)
    pack_z(1, lambda f, x: flux[2, x], fzpack)
    start(z2, None, None)
    lax.fori_loop(0, nx // 2, across_body, 0)
    start(x2, not_high_x, not_low_x)
    fypack[0] = flux[1, :, 0, :]
    fypack[1] = flux[1, :, ny - 1, :]
    start(y2, not_high_y, not_low_y)

    for inside, side in ((not_low_x, 0), (not_high_x, 1)):
        @pl.when(jnp.logical_not(inside))
        def _():
            fxhalo[side] = jnp.zeros((ny, nz), jnp.float32)
    for inside, side in ((not_low_y, 0), (not_high_y, 1)):
        @pl.when(jnp.logical_not(inside))
        def _():
            fyhalo[side] = jnp.zeros((nx, nz), jnp.float32)

    finish(zv, None, None)
    vz_joined = join_z(vzhalo)

    def source_plane(x, odd, x_low, x_high):
        fy, fz, v = flux[1, x], flux[2, x], void[x]
        y_low = jnp.where(first_row, 0.0, pltpu.roll(fy, 1, 0))
        y_high = jnp.where(last_row, 0.0, pltpu.roll(fy, ny - 1, 0))
        v_halo = unpack(vz_joined[odd], x)
        z_low = jnp.where(first_lane, 0.0, pltpu.roll(fz, 1, 1))
        z_high = jnp.where(last_lane, 0.0, pltpu.roll(fz, nz - 1, 1))
        v_low = jnp.where(first_lane, v_halo, pltpu.roll(v, 1, 1))
        v_high = jnp.where(last_lane, v_halo, pltpu.roll(v, nz - 1, 1))
        div[x] = 0.5 * ((x_high - x_low) + (y_high - y_low) + (z_high - z_low))
        slope[x] = (0.5 * time_step) * (v_high - v_low)

    def source_body(i, carry):
        x = 2 * i + 1
        source_plane(x, 1, flux[0, x - 1], flux[0, x + 1])
        source_plane(x + 1, 0, flux[0, x], flux[0, x + 2])
        return carry

    lax.fori_loop(0, nx // 2 - 1, source_body, 0)
    phase = 0
    while phase < len(phases) - 1:
        total = recv_sum(phase)
        phase += 1
        sent += send_sum(phase, total)
    finish(x2, not_high_x, not_low_x)
    source_plane(0, 0, fxhalo[0], flux[0, 1])
    source_plane(nx - 1, 1, flux[0, nx - 2], fxhalo[1])
    finish(y2, not_high_y, not_low_y)
    finish(z2, None, None)
    fz_joined = join_z(fzhalo)
    total = recv_sum(phase)
    half = line < nz // 2
    flow_sum = jnp.sum(jnp.where(half, total, 0.0), axis=1, keepdims=True)
    void_sum = jnp.sum(jnp.where(half, 0.0, total), axis=1, keepdims=True)
    cells = float(nx * ny * nz * gx * gy * gz)
    step = (target[0] * cells - flow_sum) / (time_step * void_sum)
    step_out[...] = jnp.broadcast_to(step, (1, nz)) + forcing[0]
    step = jnp.broadcast_to(step, (ny, nz))

    row_half, lane_half = row_sign / time_step, lane_sign / time_step

    def final_plane(x, odd):
        ustar[2, x] = ustar[2, x] + time_step * step
        y_halo = jnp.where(
            row < ny // 2,
            jnp.broadcast_to(fyhalo[0, pl.ds(x, 1), :], (ny, nz)),
            jnp.broadcast_to(fyhalo[1, pl.ds(x, 1), :], (ny, nz)))
        div[x] = div[x] - row_half * y_halo - lane_half * unpack(fz_joined[odd], x) + step * slope[x]

    def final_body(i, carry):
        final_plane(2 * i, 0)
        final_plane(2 * i + 1, 1)
        return carry

    lax.fori_loop(0, nx // 2, final_body, 0, unroll=2)

    for copy in sent:
        copy.wait_send()
    for pair, high, low in ((x1, not_high_x, not_low_x), (y1, not_high_y, not_low_y), (z1, None, None), (zv, None, None),
                            (x2, not_high_x, not_low_x), (y2, not_high_y, not_low_y), (z2, None, None)):
        drain(pair, high, low)


def local(velocity, pressure, voidage, particle_vel, forcing, target_flux):
    nx, ny, nz = voidage.shape
    sizes = tuple(lax.axis_size(a) for a in ("gx", "gy", "gz"))
    greet = (("gy", "gx"), ("gz",))
    if math.prod(sizes) <= DIRECT_LIMIT:
        phases = (("gz", "gy", "gx"),)
    else:
        phases = greet
    slot_count = sum(math.prod(lax.axis_size(a) for a in axes) for axes in phases)
    f32 = jnp.float32
    vmem = pl.BlockSpec(memory_space=pltpu.VMEM)
    hbm = pl.BlockSpec(memory_space=pltpu.HBM)
    dma = pltpu.SemaphoreType.DMA
    vel_new, source, forcing_new = pl.pallas_call(
        functools.partial(kernel, sizes, greet, phases),
        out_shape=(
            pltpu.VMEM((3, nx, ny, nz), f32),
            pltpu.VMEM((nx, ny, nz), f32),
            pltpu.VMEM((1, nz), f32),
        ),
        in_specs=[hbm] * 6,
        out_specs=(vmem,) * 3,
        scratch_shapes=[
            pltpu.SMEM((1,), f32),
            pltpu.SMEM((1,), f32),
            pltpu.VMEM((nx, ny, nz), f32),
            pltpu.VMEM((4, nx + 2, ny, nz), f32),
            pltpu.VMEM((nx, ny, nz), f32),
            pltpu.VMEM((3, nx, ny, nz), f32),
            pltpu.VMEM((nx, ny, nz), f32),
            pltpu.VMEM((3, nx, ny, nz), f32),
            pltpu.VMEM((2, 4, nx, nz), f32),
            pltpu.VMEM((2, 4, nx, nz), f32),
            pltpu.VMEM((2, ny, nz), f32),
            pltpu.VMEM((2, ny, nz), f32),
            pltpu.VMEM((2, nx, nz), f32),
            pltpu.VMEM((2, nx, nz), f32),
            pltpu.VMEM((2, ny, nz), f32),
            pltpu.VMEM((2, ny, nz), f32),
            pltpu.VMEM((2, ny, nz), f32),
            pltpu.VMEM((2, ny, nz), f32),
            pltpu.VMEM((2, ny, nz), f32),
            pltpu.VMEM((slot_count, 1, nz), f32),
            dma((6,)), dma((8,)), dma((8,)), dma((6,)), dma((6,)),
            dma((slot_count,)), dma((slot_count,)),
            pltpu.SemaphoreType.REGULAR,
        ],
        compiler_params=pltpu.CompilerParams(collective_id=0, has_side_effects=True),
    )(velocity, pressure, voidage, particle_vel, forcing, target_flux)
    return vel_new, source, forcing_new[0, :1]


def solution(mesh):
    return jax.shard_map(
        local,
        mesh=mesh,
        in_specs=(
            P(None, "gx", "gy", "gz"),
            P("gx", "gy", "gz"),
            P("gx", "gy", "gz"),
            P(None, "gx", "gy", "gz"),
            P(),
            P(),
        ),
        out_specs=(P(None, "gx", "gy", "gz"), P("gx", "gy", "gz"), P()),
        check_vma=False,
    )
```
